32 devices in a mesh: groups: 2 (over y), cells: 8 (over z, x), side: 2 (over core).
Axes of the slice: x: 2, y: 2, z: 4, core: 2. Of those that a mesh axis runs over, the one named last changes fastest.
Arguments:
- datasets: float32 [2, 2000, 8192], P('side', None, ('groups', 'cells')), parts along dimension 2, may hold values from -6 to 6
- sketch: float32 [64, 8192], P(None, ('groups', 'cells')), parts along dimension 1, may hold values from -6 to 6
Outputs:
- factors: float32 [2, 64, 8192], P('side', None, ('groups', 'cells')), parts along dimension 2
The draws below stay inside these ranges and needn't reach their ends.
There are 2 independent parts, one for each index of `groups`. The reference program is written for one: setup_inputs(seed, part) draws one part's arguments, and reference() takes and returns one part's arrays. A program takes and returns all parts, laid end to end along the dimension named above; each array names one. Nothing has to cross between parts.
All inputs are finite; a program needn't handle non-finite values.
Results may differ from the reference program's by a relative error of at most 0.00009.
Values sent between devices are 32-bit elements; how exact they have to be, the bound alone decides.
A program may use at most 64 MiB of HBM per device.

```python
import jax
import jax.numpy as jnp
from jax import lax

G = 2000
K = 64
NCELLS = 4096


def shard_levels(key, dims, cuts, low, top_value):
    level = 1.0
    for dim, shards_of in cuts:
        steps = jax.random.uniform(jax.random.fold_in(jax.random.fold_in(key, 6), dim), (shards_of,), jnp.float32, low / len(cuts), top_value / len(cuts))
        level = level * jnp.repeat(jnp.exp(steps), dims[dim] // shards_of).reshape((-1,) + (1,) * (len(dims) - 1 - dim))
    return level


def scatter_about(stream_key, extent, spread, limit, split=(), kind=jnp.bfloat16):
    loudness = shard_levels(stream_key, extent, split, -0.22, 0.18) if split else 1.0
    entries = jax.random.normal(stream_key, extent, jnp.float32) * spread * loudness
    return jnp.minimum(jnp.maximum(entries, -limit), limit).astype(kind)


def setup_inputs(seed: int = 0, part: int = 0) -> dict:
    key_list = jax.random.split(jax.random.key(seed), 3)
    own_keys = jax.random.split(jax.random.fold_in(key_list[2], part), 3)
    datasets = scatter_about(own_keys[0], (2, G, NCELLS), 1.0, 6.0, ((0, 2), (2, 8)), jnp.float32)
    sketch = scatter_about(own_keys[1], (K, NCELLS), 1.0, 6.0, ((1, 8),), jnp.float32)
    return {"datasets": datasets, "sketch": sketch}


def reference(datasets, sketch):
    high = lax.Precision.HIGHEST
    first = datasets[0]
    second = datasets[1]
    panel = jnp.dot(sketch, second.T, precision=high)
    range_rows = jnp.dot(panel, first, precision=high)
    gram = jnp.dot(range_rows, range_rows.T, precision=high)
    lower = jnp.linalg.cholesky(gram)
    basis = jax.scipy.linalg.solve_triangular(lower, range_rows, lower=True)
    cross = jnp.dot(basis, first.T, precision=high)
    projected = jnp.dot(cross, second, precision=high)
    scale = jnp.sqrt(jnp.float32(NCELLS))
    return jnp.stack([basis * scale, projected / scale])
```

```python
import functools
import math

import jax
import jax.numpy as jnp
from jax import lax
from jax.experimental import pallas as pl
from jax.experimental.pallas import tpu as pltpu
from jax.sharding import PartitionSpec as P

MESH = pl.DeviceIdType.MESH
F32, BF16 = jnp.float32, jnp.bfloat16
HIGHEST = lax.Precision.HIGHEST
NT = (((1,), (1,)), ((), ()))
NN = (((1,), (0,)), ((), ()))


def each(count, body):
    if count <= 8:
        for index in range(count):
            body(index)
    else:
        lax.fori_loop(0, count, lambda index, carry: (body(index), carry)[1], 0)


def flipped(cell, bits, count):
    bit = 1
    while bit < count:
        own = lax.rem(cell // bit, 2)
        cell = cell + (bits // bit % 2) * (bit - 2 * bit * own)
        bit *= 2
    return cell


def halves(value):
    high = value.astype(BF16)
    low = (value - high.astype(F32)).astype(BF16)
    return high, low


def stacked(value):
    return jnp.concatenate(halves(value), axis=0)


def dot3(small, high, low, dims):
    rows = small.shape[0] // 2
    both = lax.dot_general(small, high, dims, preferred_element_type=F32)
    rest = lax.dot_general(small[:rows], low, dims, preferred_element_type=F32)
    return both[:rows] + (both[rows:] + rest)


def inverse_factor(gram):
    k = gram.shape[0]
    row_ids = lax.broadcasted_iota(jnp.int32, gram.shape, 0)
    lanes = lax.broadcasted_iota(jnp.int32, gram.shape, 1)
    start = jnp.where(lanes < k, (lanes == row_ids).astype(F32), gram)
    step = 8
    blocks = [start[i : i + step] for i in range(0, k, step)]
    ids = lax.broadcasted_iota(jnp.int32, (step, gram.shape[1]), 0)

    def spread(block, lane):
        return jnp.broadcast_to(block[:, lane : lane + 1], block.shape)

    for b in range(k // step):
        first = k + step * b
        block = blocks[b]
        pivot_columns = [spread(block, first + r) for r in range(step)]
        reciprocals = []
        for r in range(step):
            reciprocals.append(1.0 / pivot_columns[r][r : r + 1])
            ratio = jnp.where(ids > r, pivot_columns[r], 0.0) * reciprocals[r]
            block = block - ratio * block[r : r + 1]
            for j in range(r + 1, step):
                pivot_columns[j] = pivot_columns[j] - ratio * pivot_columns[j][r : r + 1]
        for i in range(b + 1, k // step):
            columns = [spread(blocks[i], first + r) for r in range(step)]
            below = blocks[i]
            for r in range(step):
                ratio = columns[r] * reciprocals[r]
                below = below - ratio * block[r : r + 1]
                for j in range(r + 1, step):
                    columns[j] = columns[j] - ratio * pivot_columns[j][r : r + 1]
            blocks[i] = below
        blocks[b] = block
    full = jnp.concatenate(blocks, axis=0)
    pivots = jnp.sum(jnp.where(lanes - k == row_ids, full, 0.0), axis=1, keepdims=True)
    return full / jnp.sqrt(pivots)


def kernel(
    n, owners, chunk, splits, data, sketch, out, stage, drawn, high, low, high_t, low_t, small, parts, inbox, gathered, acc, grams, total, inverse,
    load_sem, drawn_sem, part_send, part_recv, gather_send, gather_recv, gram_send, gram_recv, inv_send, inv_recv,
):
    me, side = lax.axis_index("cells"), lax.axis_index("side")
    genes, width = data.shape[1:]
    k = sketch.shape[0]
    rows = k // splits
    is_x, is_y = side == 0, side == 1
    barrier = pltpu.get_barrier_semaphore()
    paired = owners == n == 8
    first_parts = second_parts = first_gathers = second_gathers = collect_order = None
    if paired:
        first_parts = ((5, 4, 7, 6, 2, 1, 3, 0), (7, 6, 5, 1, 3, 2, 4, 0))
        second_parts = ((5, 4, 7, 6, 2, 3, 1, 0), (6, 1, 5, 4, 3, 2, 7, 0))
        first_gathers = ((5, 4, 7, 6, 3, 2, 1), (7, 6, 5, 4, 3, 2, 1))
        second_gathers = ((5, 4, 7, 6, 3, 2, 1), (7, 6, 5, 4, 3, 2, 1))
        collect_order = (0, 1, 2, 3, 4, 6, 7, 5)

    def device(cell, which):
        return {"cells": cell, "side": which}

    def cell_at(s):
        return flipped(me, s, n) if paired else lax.rem(me + s, n)

    def chunk_at(s):
        return cell_at(s) if paired else lax.rem(me + 1 + s, owners)

    def slot(s):
        return s if paired else chunk_at(s)

    def through(order, count, body, start=0, group=1):
        if order is None:
            each(count - start, lambda s: body((s + start,)))
        elif isinstance(order[0], tuple):
            inner = (me >= 2) & (me < 6)
            for test, own_order in zip((inner, jnp.logical_not(inner)), order):

                @pl.when(test)
                def _():
                    through(own_order, count, body, start, group)
        else:
            for i in range(0, len(order), group):
                body(order[i : i + group])

    def start_of(c):
        return pl.multiple_of(jnp.minimum(c * chunk, genes - chunk), 8)

    def load(s):
        return pltpu.make_async_copy(
            data.at[0, pl.ds(start_of(chunk_at(s)), chunk)], stage.at[slot(s)], load_sem.at[slot(s)]
        )

    def part_copy(h, s):
        there = s if paired else me
        return pltpu.make_async_remote_copy(
            src_ref=parts.at[h, slot(s)], dst_ref=inbox.at[h, there], send_sem=part_send.at[h, slot(s)],
            recv_sem=part_recv.at[h, there], device_id=device(chunk_at(s), 1 - side), device_id_type=MESH,
        )

    def part_arrival(h, s):
        here = s if paired else cell_at(s)
        pltpu.make_async_remote_copy(
            src_ref=parts.at[h, 0], dst_ref=inbox.at[h, here], send_sem=part_send.at[h, 0],
            recv_sem=part_recv.at[h, here], device_id=device(cell_at(s), 1 - side), device_id_type=MESH,
        ).wait_recv()
        return inbox[h, here]

    own = 0 if paired else me

    def gather_copy(h, s):
        there = s if paired else me
        return pltpu.make_async_remote_copy(
            src_ref=gathered.at[h, own], dst_ref=gathered.at[h, there], send_sem=gather_send.at[h, s],
            recv_sem=gather_recv.at[h, there], device_id=device(cell_at(s), side), device_id_type=MESH,
        )

    def gather_arrival(h, here):
        pltpu.make_async_remote_copy(
            src_ref=gathered.at[h, here], dst_ref=gathered.at[h, here], send_sem=gather_send.at[h, 0],
            recv_sem=gather_recv.at[h, here], device_id=device(me, side), device_id_type=MESH,
        ).wait_recv()

    def gram_copy(cell, where, which):
        return pltpu.make_async_remote_copy(
            src_ref=grams.at[where], dst_ref=grams.at[where], send_sem=gram_send.at[which],
            recv_sem=gram_recv.at[where], device_id=device(cell, side), device_id_type=MESH,
        )

    inverse_copy = pltpu.make_async_remote_copy(
        src_ref=inverse, dst_ref=inverse, send_sem=inv_send, recv_sem=inv_recv,
        device_id=device(me, 1 - side), device_id_type=MESH,
    )

    draw = pltpu.make_async_copy(sketch, drawn, drawn_sem)
    draw.start()
    through(first_parts, owners, lambda group: [load(s).start() for s in group])

    @pl.when(is_x)
    def _():
        each(n, lambda s: pl.semaphore_signal(
            barrier, inc=1, device_id=device(lax.rem(me + s, n), 1 - side), device_id_type=MESH
        ))

    def prepare(s):
        value = stage[slot(s)]
        twice = owners * chunk - genes
        if twice:
            c = chunk_at(s)
            ids = lax.broadcasted_iota(jnp.int32, (twice, width), 0)
            first = jnp.where(ids >= c * chunk - start_of(c), value[:twice], 0.0)
            value = jnp.concatenate([first, value[twice:]], axis=0)
        high[slot(s)], low[slot(s)] = halves(value)

    def prepare_all(group):
        for s in group:
            load(s).wait()
        for s in group:
            prepare(s)

    def prepare_and_work_out(group):
        prepare_all(group)
        values = [dot3(small[...], high[slot(s)], low[slot(s)], NT) for s in group]
        for s, value in zip(group, values):
            for h in range(splits):
                parts[h, slot(s)] = value[h * rows : (h + 1) * rows]

    def turn(c):
        high_t[c], low_t[c] = high[c].T, low[c].T

    draw.wait()

    @pl.when(is_x)
    def _():
        through(first_parts, owners, prepare_all)
        each(owners, turn)

    @pl.when(is_y)
    def _():
        small[...] = stacked(drawn[...])
        through(first_parts, owners, prepare_and_work_out, group=4)
        pl.semaphore_wait(barrier, n)
        for h in range(splits):
            through(first_parts, owners, lambda group: [part_copy(h, s).start() for s in group])

    @pl.when(me < owners)
    def _():
        for h in range(splits):

            def add(s):
                gathered[h, own] += part_arrival(h, s)

            gathered[h, own] = part_arrival(h, 0)
            each(n - 1, lambda s: add(s + 1))
            for test, order in ((is_x, first_gathers), (is_y, second_gathers)):

                @pl.when(test)
                def _():
                    through(order, n, lambda group: [gather_copy(h, s).start() for s in group], 1)

    acc[...] = jnp.zeros_like(acc)

    def collect(h, s):
        if paired:
            c = s
            if s:
                gather_arrival(h, s)
        else:
            c = lax.rem(lax.rem(me, owners) - s + owners, owners)

            @pl.when(c != me)
            def _():
                gather_arrival(h, c)

        acc[h] += dot3(stacked(gathered[h, c]), high[c], low[c], NN)

    def scatter(h, group):
        mine = small[2 * rows * h : 2 * rows * (h + 1)]
        values = [dot3(mine, high_t[slot(s)], low_t[slot(s)], NN) for s in group]
        for s, value in zip(group, values):
            parts[h, slot(s)] = value
        for s in group:
            part_copy(h, s).start()

    for h in range(splits):
        through(collect_order, owners, lambda group: [collect(h, s) for s in group])

        @pl.when(is_x)
        def _():
            small[2 * rows * h : 2 * rows * (h + 1)] = stacked(acc[h])
            through(second_parts, owners, lambda group: scatter(h, group), group=4)

    @pl.when(is_x)
    def _():
        range_rows = jnp.concatenate([acc[i] for i in range(splits)], axis=0)
        twice = lax.dot_general(
            range_rows, jnp.concatenate([range_rows, range_rows], axis=0), NT,
            precision=HIGHEST, preferred_element_type=F32,
        )
        left = lax.broadcasted_iota(jnp.int32, grams.shape[1:], 1) < k
        grams[me] = jnp.where(left, twice[: k // 2], twice[k // 2 :])
        each(n - 1, lambda s: gram_copy(lax.rem(me + 1 + s, n), me, s).start())

        def arrive(s):
            gram_copy(me, lax.rem(me - 1 - s + n, n), 0).wait_recv()

        each(n - 1, arrive)
        total[...] = grams[0]

        def add(i):
            total[...] += grams[i + 1]

        each(n - 1, add)
        bottom = total[...]
        gram = jnp.concatenate([pltpu.roll(bottom, k, axis=1), bottom], axis=0)
        inverse[...] = inverse_factor(gram)
        inverse_copy.start()

    @pl.when(is_y)
    def _():
        inverse_copy.wait_recv()

    scale = math.sqrt(width * n)
    factor = jnp.where(is_x, scale, 1.0 / scale).astype(F32)
    full = jnp.concatenate([acc[h] for h in range(splits)], axis=0)
    out[0] = factor * dot3(stacked(inverse[:, :k]), *halves(full), NN)

    for h in range(splits):
        each(owners, lambda s: part_copy(h, s).wait_send())

        @pl.when(me < owners)
        def _():
            each(n - 1, lambda s: gather_copy(h, s + 1).wait_send())

    @pl.when(is_x)
    def _():
        each(n - 1, lambda s: gram_copy(lax.rem(me + 1 + s, n), me, s).wait_send())
        inverse_copy.wait_send()


def solution(mesh):
    n = mesh.shape["cells"]

    def per_device(datasets, sketch):
        genes, width = datasets.shape[1:]
        k = sketch.shape[0]
        chunk = 128 * -(-genes // (128 * n))
        owners = -(-genes // chunk)
        splits = 2 if owners == n == 8 and k % 16 == 0 else 1
        rows = k // splits
        dma = pltpu.SemaphoreType.DMA
        return pl.pallas_call(
            functools.partial(kernel, n, owners, chunk, splits),
            out_shape=jax.ShapeDtypeStruct((1, k, width), F32),
            in_specs=[pl.BlockSpec(memory_space=pl.ANY)] * 2,
            out_specs=pl.BlockSpec(memory_space=pltpu.VMEM),
            scratch_shapes=[
                pltpu.VMEM((owners, chunk, width), F32),
                pltpu.VMEM((k, width), F32),
                pltpu.VMEM((owners, chunk, width), BF16),
                pltpu.VMEM((owners, chunk, width), BF16),
                pltpu.VMEM((owners, width, chunk), BF16),
                pltpu.VMEM((owners, width, chunk), BF16),
                pltpu.VMEM((2 * k, width), BF16),
                pltpu.VMEM((splits, owners, rows, chunk), F32),
                pltpu.VMEM((splits, n, rows, chunk), F32),
                pltpu.VMEM((splits, owners, rows, chunk), F32),
                pltpu.VMEM((splits, rows, width), F32),
                pltpu.VMEM((n, k // 2, 2 * k), F32),
                pltpu.VMEM((k // 2, 2 * k), F32),
                pltpu.VMEM((k, 2 * k), F32),
                dma((owners,)), dma,
                dma((splits, owners)), dma((splits, n)),
                dma((splits, n)), dma((splits, owners)),
                dma((n,)), dma((n,)),
                dma, dma,
            ],
            compiler_params=pltpu.CompilerParams(collective_id=0, has_side_effects=True),
            name="power_pass",
        )(datasets, sketch)

    spec = P("side", None, ("groups", "cells"))
    return jax.shard_map(
        per_device, mesh=mesh, in_specs=(spec, P(None, ("groups", "cells"))), out_specs=spec, check_vma=False
    )
```

```python
import functools
import math

import jax
import jax.numpy as jnp
from jax import lax
from jax.experimental import pallas as pl
from jax.experimental.pallas import tpu as pltpu
from jax.sharding import PartitionSpec as P

MESH = pl.DeviceIdType.MESH
F32, BF16 = jnp.float32, jnp.bfloat16
HIGHEST = lax.Precision.HIGHEST
NT = (((1,), (1,)), ((), ()))
NN = (((1,), (0,)), ((), ()))


def each(count, body):
    if count <= 8:
        for index in range(count):
            body(index)
    else:
        lax.fori_loop(0, count, lambda index, carry: (body(index), carry)[1], 0)


def flipped(cell, bits, count):
    bit = 1
    while bit < count:
        own = lax.rem(cell // bit, 2)
        cell = cell + (bits // bit % 2) * (bit - 2 * bit * own)
        bit *= 2
    return cell


def halves(value):
    high = value.astype(BF16)
    low = (value - high.astype(F32)).astype(BF16)
    return high, low


def stacked(value):
    return jnp.concatenate(halves(value), axis=0)


def dot3(small, high, low, dims):
    rows = small.shape[0] // 2
    both = lax.dot_general(small, high, dims, preferred_element_type=F32)
    rest = lax.dot_general(small[:rows], low, dims, preferred_element_type=F32)
    return both[:rows] + (both[rows:] + rest)


def inverse_factor(gram):
    k = gram.shape[0]
    row_ids = lax.broadcasted_iota(jnp.int32, gram.shape, 0)
    lanes = lax.broadcasted_iota(jnp.int32, gram.shape, 1)
    start = jnp.where(lanes < k, (lanes == row_ids).astype(F32), gram)
    step = 8
    blocks = [start[i : i + step] for i in range(0, k, step)]
    ids = lax.broadcasted_iota(jnp.int32, (step, gram.shape[1]), 0)

    def spread(block, lane):
        return jnp.broadcast_to(block[:, lane : lane + 1], block.shape)

    for b in range(k // step):
        first = k + step * b
        block = blocks[b]
        pivot_columns = [spread(block, first + r) for r in range(step)]
        reciprocals = []
        for r in range(step):
            reciprocals.append(1.0 / pivot_columns[r][r : r + 1])
            ratio = jnp.where(ids > r, pivot_columns[r], 0.0) * reciprocals[r]
            block = block - ratio * block[r : r + 1]
            for j in range(r + 1, step):
                pivot_columns[j] = pivot_columns[j] - ratio * pivot_columns[j][r : r + 1]
        for i in range(b + 1, k // step):
            columns = [spread(blocks[i], first + r) for r in range(step)]
            below = blocks[i]
            for r in range(step):
                ratio = columns[r] * reciprocals[r]
                below = below - ratio * block[r : r + 1]
                for j in range(r + 1, step):
                    columns[j] = columns[j] - ratio * pivot_columns[j][r : r + 1]
            blocks[i] = below
        blocks[b] = block
    full = jnp.concatenate(blocks, axis=0)
    pivots = jnp.sum(jnp.where(lanes - k == row_ids, full, 0.0), axis=1, keepdims=True)
    return full / jnp.sqrt(pivots)


def kernel(
    n, owners, chunk, splits, data, sketch, out, stage, drawn, high, low, high_t, low_t, small, parts, inbox, gathered, acc, grams, total, inverse,
    load_sem, drawn_sem, part_send, part_recv, gather_send, gather_recv, gram_send, gram_recv, inv_send, inv_recv,
):
    me, side = lax.axis_index("cells"), lax.axis_index("side")
    genes, width = data.shape[1:]
    k = sketch.shape[0]
    rows = k // splits
    is_x, is_y = side == 0, side == 1
    barrier = pltpu.get_barrier_semaphore()
    paired = owners == n == 8
    first_parts = second_parts = first_gathers = second_gathers = collect_order = None
    if paired:
        first_parts = ((5, 4, 7, 6, 2, 1, 3, 0), (7, 6, 5, 1, 3, 2, 4, 0))
        second_parts = ((5, 4, 7, 6, 2, 3, 1, 0), (6, 1, 5, 4, 3, 2, 7, 0))
        first_gathers = ((5, 4, 7, 6, 3, 2, 1), (7, 6, 5, 4, 3, 2, 1))
        second_gathers = ((5, 4, 7, 6, 3, 2, 1), (7, 6, 5, 4, 3, 2, 1))
        collect_order = (0, 1, 2, 3, 4, 6, 7, 5)

    def device(cell, which):
        return {"cells": cell, "side": which}

    def cell_at(s):
        return flipped(me, s, n) if paired else lax.rem(me + s, n)

    def chunk_at(s):
        return cell_at(s) if paired else lax.rem(me + 1 + s, owners)

    def slot(s):
        return s if paired else chunk_at(s)

    def through(order, count, body, start=0, group=1):
        if order is None:
            each(count - start, lambda s: body((s + start,)))
        elif isinstance(order[0], tuple):
            inner = (me >= 2) & (me < 6)
            for test, own_order in zip((inner, jnp.logical_not(inner)), order):

                @pl.when(test)
                def _():
                    through(own_order, count, body, start, group)
        else:
            for i in range(0, len(order), group):
                body(order[i : i + group])

    def start_of(c):
        return pl.multiple_of(jnp.minimum(c * chunk, genes - chunk), 8)

    def load(s):
        return pltpu.make_async_copy(
            data.at[0, pl.ds(start_of(chunk_at(s)), chunk)], stage.at[slot(s)], load_sem.at[slot(s)]
        )

    def part_copy(h, s):
        there = s if paired else me
        return pltpu.make_async_remote_copy(
            src_ref=parts.at[h, slot(s)], dst_ref=inbox.at[h, there], send_sem=part_send.at[h, slot(s)],
            recv_sem=part_recv.at[h, there], device_id=device(chunk_at(s), 1 - side), device_id_type=MESH,
        )

    def part_arrival(h, s):
        here = s if paired else cell_at(s)
        pltpu.make_async_remote_copy(
            src_ref=parts.at[h, 0], dst_ref=inbox.at[h, here], send_sem=part_send.at[h, 0],
            recv_sem=part_recv.at[h, here], device_id=device(cell_at(s), 1 - side), device_id_type=MESH,
        ).wait_recv()
        return inbox[h, here]

    own = 0 if paired else me

    def gather_copy(h, s):
        there = s if paired else me
        return pltpu.make_async_remote_copy(
            src_ref=gathered.at[h, own], dst_ref=gathered.at[h, there], send_sem=gather_send.at[h, s],
            recv_sem=gather_recv.at[h, there], device_id=device(cell_at(s), side), device_id_type=MESH,
        )

    def gather_arrival(h, here):
        pltpu.make_async_remote_copy(
            src_ref=gathered.at[h, here], dst_ref=gathered.at[h, here], send_sem=gather_send.at[h, 0],
            recv_sem=gather_recv.at[h, here], device_id=device(me, side), device_id_type=MESH,
        ).wait_recv()

    def gram_copy(cell, where, which):
        return pltpu.make_async_remote_copy(
            src_ref=grams.at[where], dst_ref=grams.at[where], send_sem=gram_send.at[which],
            recv_sem=gram_recv.at[where], device_id=device(cell, side), device_id_type=MESH,
        )

    inverse_copy = pltpu.make_async_remote_copy(
        src_ref=inverse, dst_ref=inverse, send_sem=inv_send, recv_sem=inv_recv,
        device_id=device(me, 1 - side), device_id_type=MESH,
    )

    draw = pltpu.make_async_copy(sketch, drawn, drawn_sem)
    draw.start()
    through(first_parts, owners, lambda group: [load(s).start() for s in group])

    @pl.when(is_x)
    def _():
        each(n, lambda s: pl.semaphore_signal(
            barrier, inc=1, device_id=device(lax.rem(me + s, n), 1 - side), device_id_type=MESH
        ))

    def prepare(s):
        value = stage[slot(s)]
        twice = owners * chunk - genes
        if twice:
            c = chunk_at(s)
            ids = lax.broadcasted_iota(jnp.int32, (twice, width), 0)
            first = jnp.where(ids >= c * chunk - start_of(c), value[:twice], 0.0)
            value = jnp.concatenate([first, value[twice:]], axis=0)
        high[slot(s)], low[slot(s)] = halves(value)

    def prepare_all(group):
        for s in group:
            load(s).wait()
        for s in group:
            prepare(s)

    def prepare_and_work_out(group):
        prepare_all(group)
        values = [dot3(small[...], high[slot(s)], low[slot(s)], NT) for s in group]
        for s, value in zip(group, values):
            for h in range(splits):
                parts[h, slot(s)] = value[h * rows : (h + 1) * rows]

    def turn(c):
        high_t[c], low_t[c] = high[c].T, low[c].T

    draw.wait()

    @pl.when(is_x)
    def _():
        through(first_parts, owners, prepare_all)
        each(owners, turn)

    @pl.when(is_y)
    def _():
        small[...] = stacked(drawn[...])
        through(first_parts, owners, prepare_and_work_out, group=4)
        pl.semaphore_wait(barrier, n)
        for h in range(splits):
            through(first_parts, owners, lambda group: [part_copy(h, s).start() for s in group])

    @pl.when(me < owners)
    def _():
        for h in range(splits):

            def add(s):
                gathered[h, own] += part_arrival(h, s)

            gathered[h, own] = part_arrival(h, 0)
            each(n - 1, lambda s: add(s + 1))
            for test, order in ((is_x, first_gathers), (is_y, second_gathers)):

                @pl.when(test)
                def _():
                    through(order, n, lambda group: [gather_copy(h, s).start() for s in group], 1)

    acc[...] = jnp.zeros_like(acc)

    def collect(h, s):
        if paired:
            c = s
            if s:
                gather_arrival(h, s)
        else:
            c = lax.rem(lax.rem(me, owners) - s + owners, owners)

            @pl.when(c != me)
            def _():
                gather_arrival(h, c)

        acc[h] += dot3(stacked(gathered[h, c]), high[c], low[c], NN)

    def scatter(h, group):
        mine = small[2 * rows * h : 2 * rows * (h + 1)]
        values = [dot3(mine, high_t[slot(s)], low_t[slot(s)], NN) for s in group]
        for s, value in zip(group, values):
            parts[h, slot(s)] = value
        for s in group:
            part_copy(h, s).start()

    for h in range(splits):
        through(collect_order, owners, lambda group: [collect(h, s) for s in group])

        @pl.when(is_x)
        def _():
            small[2 * rows * h : 2 * rows * (h + 1)] = stacked(acc[h])
            through(second_parts, owners, lambda group: scatter(h, group), group=4)

    @pl.when(is_x)
    def _():
        range_rows = jnp.concatenate([acc[i] for i in range(splits)], axis=0)
        twice = lax.dot_general(
            range_rows, jnp.concatenate([range_rows, range_rows], axis=0), NT,
            precision=HIGHEST, preferred_element_type=F32,
        )
        left = lax.broadcasted_iota(jnp.int32, grams.shape[1:], 1) < k
        grams[me] = jnp.where(left, twice[: k // 2], twice[k // 2 :])
        each(n - 1, lambda s: gram_copy(lax.rem(me + 1 + s, n), me, s).start())

        def arrive(s):
            gram_copy(me, lax.rem(me - 1 - s + n, n), 0).wait_recv()

        each(n - 1, arrive)
        total[...] = grams[0]

        def add(i):
            total[...] += grams[i + 1]

        each(n - 1, add)
        bottom = total[...]
        gram = jnp.concatenate([pltpu.roll(bottom, k, axis=1), bottom], axis=0)
        inverse[...] = inverse_factor(gram)
        inverse_copy.start()

    @pl.when(is_y)
    def _():
        inverse_copy.wait_recv()

    scale = math.sqrt(width * n)
    factor = jnp.where(is_x, scale, 1.0 / scale).astype(F32)
    full = jnp.concatenate([acc[h] for h in range(splits)], axis=0)
    out[0] = factor * dot3(stacked(inverse[:, :k]), *halves(full), NN)

    for h in range(splits):
        each(owners, lambda s: part_copy(h, s).wait_send())

        @pl.when(me < owners)
        def _():
            each(n - 1, lambda s: gather_copy(h, s + 1).wait_send())

    @pl.when(is_x)
    def _():
        each(n - 1, lambda s: gram_copy(lax.rem(me + 1 + s, n), me, s).wait_send())
        inverse_copy.wait_send()


def solution(mesh):
    n = mesh.shape["cells"]

    def per_device(datasets, sketch):
        genes, width = datasets.shape[1:]
        k = sketch.shape[0]
        chunk = 128 * -(-genes // (128 * n))
        owners = -(-genes // chunk)
        splits = 2 if owners == n == 8 and k % 16 == 0 else 1
        rows = k // splits
        dma = pltpu.SemaphoreType.DMA
        return pl.pallas_call(
            functools.partial(kernel, n, owners, chunk, splits),
            out_shape=pltpu.VMEM((1, k, width), F32),
            in_specs=[pl.BlockSpec(memory_space=pl.ANY)] * 2,
            out_specs=pl.BlockSpec(memory_space=pltpu.VMEM),
            scratch_shapes=[
                pltpu.VMEM((owners, chunk, width), F32),
                pltpu.VMEM((k, width), F32),
                pltpu.VMEM((owners, chunk, width), BF16),
                pltpu.VMEM((owners, chunk, width), BF16),
                pltpu.VMEM((owners, width, chunk), BF16),
                pltpu.VMEM((owners, width, chunk), BF16),
                pltpu.VMEM((2 * k, width), BF16),
                pltpu.VMEM((splits, owners, rows, chunk), F32),
                pltpu.VMEM((splits, n, rows, chunk), F32),
                pltpu.VMEM((splits, owners, rows, chunk), F32),
                pltpu.VMEM((splits, rows, width), F32),
                pltpu.VMEM((n, k // 2, 2 * k), F32),
                pltpu.VMEM((k // 2, 2 * k), F32),
                pltpu.VMEM((k, 2 * k), F32),
                dma((owners,)), dma,
                dma((splits, owners)), dma((splits, n)),
                dma((splits, n)), dma((splits, owners)),
                dma((n,)), dma((n,)),
                dma, dma,
            ],
            compiler_params=pltpu.CompilerParams(collective_id=0, has_side_effects=True),
            name="power_pass",
        )(datasets, sketch)

    spec = P("side", None, ("groups", "cells"))
    return jax.shard_map(
        per_device, mesh=mesh, in_specs=(spec, P(None, ("groups", "cells"))), out_specs=spec, check_vma=False
    )
```

```python
import functools
import math

import jax
import jax.numpy as jnp
from jax import lax
from jax.experimental import pallas as pl
from jax.experimental.pallas import tpu as pltpu
from jax.sharding import PartitionSpec as P

MESH = pl.DeviceIdType.MESH
F32, BF16 = jnp.float32, jnp.bfloat16
HIGHEST = lax.Precision.HIGHEST
NT = (((1,), (1,)), ((), ()))
NN = (((1,), (0,)), ((), ()))


def each(count, body):
    if count <= 8:
        for index in range(count):
            body(index)
    else:
        lax.fori_loop(0, count, lambda index, carry: (body(index), carry)[1], 0)


def flipped(cell, bits, count):
    bit = 1
    while bit < count:
        own = lax.rem(cell // bit, 2)
        cell = cell + (bits // bit % 2) * (bit - 2 * bit * own)
        bit *= 2
    return cell


def halves(value):
    high = value.astype(BF16)
    low = (value - high.astype(F32)).astype(BF16)
    return high, low


def stacked(value):
    return jnp.concatenate(halves(value), axis=0)


def dot3(small, high, low, dims):
    rows = small.shape[0] // 2
    both = lax.dot_general(small, high, dims, preferred_element_type=F32)
    rest = lax.dot_general(small[:rows], low, dims, preferred_element_type=F32)
    return both[:rows] + (both[rows:] + rest)


def inverse_factor(gram):
    k = gram.shape[0]
    row_ids = lax.broadcasted_iota(jnp.int32, gram.shape, 0)
    lanes = lax.broadcasted_iota(jnp.int32, gram.shape, 1)
    start = jnp.where(lanes < k, (lanes == row_ids).astype(F32), gram)
    step = 8
    blocks = [start[i : i + step] for i in range(0, k, step)]
    ids = lax.broadcasted_iota(jnp.int32, (step, gram.shape[1]), 0)

    def spread(block, lane):
        return jnp.broadcast_to(block[:, lane : lane + 1], block.shape)

    for b in range(k // step):
        first = k + step * b
        block = blocks[b]
        pivot_columns = [spread(block, first + r) for r in range(step)]
        reciprocals = []
        for r in range(step):
            reciprocals.append(1.0 / pivot_columns[r][r : r + 1])
            ratio = jnp.where(ids > r, pivot_columns[r], 0.0) * reciprocals[r]
            block = block - ratio * block[r : r + 1]
            for j in range(r + 1, step):
                pivot_columns[j] = pivot_columns[j] - ratio * pivot_columns[j][r : r + 1]
        for i in range(b + 1, k // step):
            columns = [spread(blocks[i], first + r) for r in range(step)]
            below = blocks[i]
            for r in range(step):
                ratio = columns[r] * reciprocals[r]
                below = below - ratio * block[r : r + 1]
                for j in range(r + 1, step):
                    columns[j] = columns[j] - ratio * pivot_columns[j][r : r + 1]
            blocks[i] = below
        blocks[b] = block
    full = jnp.concatenate(blocks, axis=0)
    pivots = jnp.sum(jnp.where(lanes - k == row_ids, full, 0.0), axis=1, keepdims=True)
    return full / jnp.sqrt(pivots)


def kernel(
    n, owners, chunk, splits, data, sketch, out, stage, drawn, high, low, high_t, low_t, small, parts, inbox, gathered, acc, grams, total, inverse,
    passing, load_sem, drawn_sem, part_send, part_recv, pass_recv, gather_send, gather_recv, gram_send, gram_recv, inv_send, inv_recv,
):
    me, side = lax.axis_index("cells"), lax.axis_index("side")
    genes, width = data.shape[1:]
    k = sketch.shape[0]
    rows = k // splits
    is_x, is_y = side == 0, side == 1
    barrier = pltpu.get_barrier_semaphore()
    paired = owners == n == 8
    loads = first_sends = second_parts = first_gathers = second_gathers = first_collect = second_collect = None
    relayed_parts = relayed_gathers = ()
    if paired:
        loads = ((5, 4, 7, 6, 2, 1, 3, 0), (7, 6, 5, 1, 3, 2, 4, 0))
        first_sends = (
            (5, 4, 7, 6, 2, 1, 3, 0, 13, 12, 15, 14, 10, 9, 11, 8),
            (7, 6, 5, 1, 3, 2, 4, 0, 15, 14, 13, 9, 11, 10, 12, 8),
        )
        second_parts = ((5, 4, 7, 6, 2, 3, 1, 0), (6, 1, 5, 4, 3, 2, 7, 0))
        first_gathers = ((5, 4, 7, 6, 3, 2, 1), (7, 6, 5, 4, 3, 2, 1))
        second_gathers = ((5, 4, 7, 6, 3, 2, 1), (7, 6, 5, 4, 3, 2, 1))
        first_collect = (0, 1, 2, 3, 4, 6, 7, 5)
        second_collect = (0, 1, 2, 3, 4, 6, 7, 5)
        relayed_parts = ()
        relayed_gathers = ()

    def device(cell, which):
        return {"cells": cell, "side": which}

    def cell_at(s):
        return flipped(me, s, n) if paired else lax.rem(me + s, n)

    def chunk_at(s):
        return cell_at(s) if paired else lax.rem(me + 1 + s, owners)

    def slot(s):
        return s if paired else chunk_at(s)

    def through(order, count, body, start=0, group=1):
        if order is None:
            each(count - start, lambda s: body((s + start,)))
        elif isinstance(order[0], tuple):
            inner = (me >= 2) & (me < 6)
            for test, own_order in zip((inner, jnp.logical_not(inner)), order):

                @pl.when(test)
                def _():
                    through(own_order, count, body, start, group)
        else:
            for i in range(0, len(order), group):
                body(order[i : i + group])

    def start_of(c):
        return pl.multiple_of(jnp.minimum(c * chunk, genes - chunk), 8)

    def load(s):
        return pltpu.make_async_copy(
            data.at[0, pl.ds(start_of(chunk_at(s)), chunk)], stage.at[slot(s)], load_sem.at[slot(s)]
        )

    def part_copy(h, s):
        there = s if paired else me
        return pltpu.make_async_remote_copy(
            src_ref=parts.at[h, slot(s)], dst_ref=inbox.at[h, there], send_sem=part_send.at[h, slot(s)],
            recv_sem=part_recv.at[h, there], device_id=device(chunk_at(s), 1 - side), device_id_type=MESH,
        )

    def part_arrival(h, s):
        here = s if paired else cell_at(s)
        pltpu.make_async_remote_copy(
            src_ref=parts.at[h, 0], dst_ref=inbox.at[h, here], send_sem=part_send.at[h, 0],
            recv_sem=part_recv.at[h, here], device_id=device(cell_at(s), 1 - side), device_id_type=MESH,
        ).wait_recv()
        return inbox[h, here]

    def relay_part(h, s):
        return pltpu.make_async_remote_copy(
            src_ref=parts.at[h, s], dst_ref=passing.at[h, s - 1], send_sem=part_send.at[h, s],
            recv_sem=pass_recv.at[h, s - 1], device_id=device(cell_at(1), side), device_id_type=MESH,
        )

    own = 0 if paired else me

    def gather_copy(h, s):
        there = s if paired else me
        return pltpu.make_async_remote_copy(
            src_ref=gathered.at[h, own], dst_ref=gathered.at[h, there], send_sem=gather_send.at[h, s],
            recv_sem=gather_recv.at[h, there], device_id=device(cell_at(s), side), device_id_type=MESH,
        )

    def gather_arrival(h, here):
        pltpu.make_async_remote_copy(
            src_ref=gathered.at[h, here], dst_ref=gathered.at[h, here], send_sem=gather_send.at[h, 0],
            recv_sem=gather_recv.at[h, here], device_id=device(me, side), device_id_type=MESH,
        ).wait_recv()

    def relay_gather(h, s):
        return pltpu.make_async_remote_copy(
            src_ref=gathered.at[h, s], dst_ref=gathered.at[h, s + 1], send_sem=gather_send.at[h, s + 1],
            recv_sem=gather_recv.at[h, s + 1], device_id=device(cell_at(1), side), device_id_type=MESH,
        )

    def gram_copy(cell, where, which):
        return pltpu.make_async_remote_copy(
            src_ref=grams.at[where], dst_ref=grams.at[where], send_sem=gram_send.at[which],
            recv_sem=gram_recv.at[where], device_id=device(cell, side), device_id_type=MESH,
        )

    inverse_copy = pltpu.make_async_remote_copy(
        src_ref=inverse, dst_ref=inverse, send_sem=inv_send, recv_sem=inv_recv,
        device_id=device(me, 1 - side), device_id_type=MESH,
    )

    draw = pltpu.make_async_copy(sketch, drawn, drawn_sem)
    draw.start()
    through(loads, owners, lambda group: [load(s).start() for s in group])

    @pl.when(is_x)
    def _():
        each(n, lambda s: pl.semaphore_signal(
            barrier, inc=1, device_id=device(lax.rem(me + s, n), 1 - side), device_id_type=MESH
        ))

    if relayed_parts:

        @pl.when(is_y)
        def _():
            pl.semaphore_signal(barrier, inc=1, device_id=device(cell_at(1), side), device_id_type=MESH)

    def send_first(h, s):
        if s in relayed_parts:
            relay_part(h, s).start()
            return
        if s + 1 in relayed_parts:
            relay_part(h, s + 1).wait_recv()
            parts[h, s] += passing[h, s]
        part_copy(h, s).start()

    def prepare(s):
        value = stage[slot(s)]
        twice = owners * chunk - genes
        if twice:
            c = chunk_at(s)
            ids = lax.broadcasted_iota(jnp.int32, (twice, width), 0)
            first = jnp.where(ids >= c * chunk - start_of(c), value[:twice], 0.0)
            value = jnp.concatenate([first, value[twice:]], axis=0)
        high[slot(s)], low[slot(s)] = halves(value)

    def prepare_all(group):
        for s in group:
            load(s).wait()
        for s in group:
            prepare(s)

    def prepare_and_work_out(group):
        prepare_all(group)
        values = [dot3(small[...], high[slot(s)], low[slot(s)], NT) for s in group]
        for s, value in zip(group, values):
            for h in range(splits):
                parts[h, slot(s)] = value[h * rows : (h + 1) * rows]

    def turn(c):
        high_t[c], low_t[c] = high[c].T, low[c].T

    draw.wait()

    @pl.when(is_x)
    def _():
        through(loads, owners, prepare_all)
        each(owners, turn)

    @pl.when(is_y)
    def _():
        small[...] = stacked(drawn[...])
        through(loads, owners, prepare_and_work_out, group=4)
        pl.semaphore_wait(barrier, n + 1 if relayed_parts else n)
        if paired:
            through(first_sends, splits * owners, lambda group: [send_first(*divmod(t, owners)) for t in group])
        else:
            each(owners, lambda s: part_copy(0, s).start())

    def total_up(skipped, order):
        for h in range(splits):

            def add(s):
                gathered[h, own] += part_arrival(h, s)

            gathered[h, own] = part_arrival(h, 0)
            if paired:
                for s in (1, 2, 3, 6, 7, 4, 5):
                    if s not in skipped:
                        add(s)
            else:
                each(n - 1, lambda s: add(s + 1))
            through(order, n, lambda group: [gather_copy(h, s).start() for s in group], 1)

    @pl.when(is_x & (me < owners))
    def _():
        total_up(relayed_parts, first_gathers)

    @pl.when(is_y & (me < owners))
    def _():
        total_up((), second_gathers)

    acc[...] = jnp.zeros_like(acc)

    def collect(h, s, relayed):
        if paired:
            c = s
            if s:
                gather_arrival(h, s)
            if s + 1 in relayed:
                relay_gather(h, s).start()
        else:
            c = lax.rem(lax.rem(me, owners) - s + owners, owners)

            @pl.when(c != me)
            def _():
                gather_arrival(h, c)

        acc[h] += dot3(stacked(gathered[h, c]), high[c], low[c], NN)

    lanes = lax.broadcasted_iota(jnp.int32, grams.shape[1:], 1)

    def work_out_gram():
        if splits == 2:
            products = lax.dot_general(small[...], small[...], NT, preferred_element_type=F32)
            pair = [products[2 * rows * h : 2 * rows * h + rows] + products[2 * rows * h + rows : 2 * rows * (h + 1)] for h in range(2)]
            top, bottom = [value + pltpu.roll(value, 2 * k - rows, axis=1) for value in pair]
            grams[me] = jnp.where(lax.rem(lanes, k) < rows, top, pltpu.roll(bottom, rows, axis=1))
            return
        range_rows = jnp.concatenate([acc[i] for i in range(splits)], axis=0)
        twice = lax.dot_general(
            range_rows, jnp.concatenate([range_rows, range_rows], axis=0), NT,
            precision=HIGHEST, preferred_element_type=F32,
        )
        grams[me] = jnp.where(lanes < k, twice[: k // 2], twice[k // 2 :])

    def send_gram():
        each(n - 1, lambda s: gram_copy(lax.rem(me + 1 + s, n), me, s).start())

    def scatter(h, group, with_gram):
        mine = small[2 * rows * h : 2 * rows * (h + 1)]
        values = [dot3(mine, high_t[slot(s)], low_t[slot(s)], NN) for s in group]
        if with_gram:
            work_out_gram()
        for s, value in zip(group, values):
            parts[h, slot(s)] = value
        if with_gram:
            send_gram()
        for s in group:
            part_copy(h, s).start()

    def scatter_all(h, order):
        for i in range(0, owners, 4):
            scatter(h, order[i : i + 4], h == splits - 1 and i == 4)

    @pl.when(is_x)
    def _():
        for h in range(splits):
            if paired:
                for s in first_collect:
                    collect(h, s, ())
            else:
                each(owners, lambda s: collect(h, s, ()))
            small[2 * rows * h : 2 * rows * (h + 1)] = stacked(acc[h])
            if paired:
                through(second_parts, owners, lambda order: scatter_all(h, order), group=owners)
            else:
                each(owners, lambda s: scatter(h, (s,), False))
        if not paired:
            work_out_gram()
            send_gram()

        def arrive(s):
            gram_copy(me, lax.rem(me - 1 - s + n, n), 0).wait_recv()

        each(n - 1, arrive)
        total[...] = grams[0]

        def add(i):
            total[...] += grams[i + 1]

        each(n - 1, add)
        top = bottom = total[...]
        if splits == 2:
            top = jnp.where(lanes < rows, top, pltpu.roll(top, k + rows, axis=1))
            bottom = jnp.where(lanes < k + rows, pltpu.roll(bottom, rows, axis=1), bottom)
        gram = jnp.concatenate([pltpu.roll(top, k, axis=1), bottom], axis=0)
        inverse[...] = inverse_factor(gram)
        inverse_copy.start()

    @pl.when(is_y)
    def _():
        for h in range(splits):
            if paired:
                for s in second_collect:
                    collect(h, s, relayed_gathers)
            else:
                each(owners, lambda s: collect(h, s, ()))
        inverse_copy.wait_recv()

    scale = math.sqrt(width * n)
    factor = jnp.where(is_x, scale, 1.0 / scale).astype(F32)
    full = jnp.concatenate([acc[h] for h in range(splits)], axis=0)
    out[0] = factor * dot3(stacked(inverse[:, :k]), *halves(full), NN)

    for h in range(splits):
        each(owners, lambda s: part_copy(h, s).wait_send())

        @pl.when(me < owners)
        def _():
            each(n - 1, lambda s: gather_copy(h, s + 1).wait_send())

    @pl.when(is_x)
    def _():
        each(n - 1, lambda s: gram_copy(lax.rem(me + 1 + s, n), me, s).wait_send())
        inverse_copy.wait_send()


def solution(mesh):
    n = mesh.shape["cells"]

    def per_device(datasets, sketch):
        genes, width = datasets.shape[1:]
        k = sketch.shape[0]
        chunk = 128 * -(-genes // (128 * n))
        owners = -(-genes // chunk)
        splits = 2 if owners == n == 8 and k % 16 == 0 else 1
        rows = k // splits
        dma = pltpu.SemaphoreType.DMA
        return pl.pallas_call(
            functools.partial(kernel, n, owners, chunk, splits),
            out_shape=pltpu.VMEM((1, k, width), F32),
            in_specs=[pl.BlockSpec(memory_space=pl.ANY)] * 2,
            out_specs=pl.BlockSpec(memory_space=pltpu.VMEM),
            scratch_shapes=[
                pltpu.VMEM((owners, chunk, width), F32),
                pltpu.VMEM((k, width), F32),
                pltpu.VMEM((owners, chunk, width), BF16),
                pltpu.VMEM((owners, chunk, width), BF16),
                pltpu.VMEM((owners, width, chunk), BF16),
                pltpu.VMEM((owners, width, chunk), BF16),
                pltpu.VMEM((2 * k, width), BF16),
                pltpu.VMEM((splits, owners, rows, chunk), F32),
                pltpu.VMEM((splits, n, rows, chunk), F32),
                pltpu.VMEM((splits, owners, rows, chunk), F32),
                pltpu.VMEM((splits, rows, width), F32),
                pltpu.VMEM((n, k // 2, 2 * k), F32),
                pltpu.VMEM((k // 2, 2 * k), F32),
                pltpu.VMEM((k, 2 * k), F32),
                pltpu.VMEM((splits, owners, rows, chunk), F32),
                dma((owners,)), dma,
                dma((splits, owners)), dma((splits, n)), dma((splits, owners)),
                dma((splits, n)), dma((splits, owners)),
                dma((n,)), dma((n,)),
                dma, dma,
            ],
            compiler_params=pltpu.CompilerParams(collective_id=0, has_side_effects=True),
            name="power_pass",
        )(datasets, sketch)

    spec = P("side", None, ("groups", "cells"))
    return jax.shard_map(
        per_device, mesh=mesh, in_specs=(spec, P(None, ("groups", "cells"))), out_specs=spec, check_vma=False
    )
```

```python
import functools
import math

import jax
import jax.numpy as jnp
from jax import lax
from jax.experimental import pallas as pl
from jax.experimental.pallas import tpu as pltpu
from jax.sharding import PartitionSpec as P

MESH = pl.DeviceIdType.MESH
F32, BF16 = jnp.float32, jnp.bfloat16
HIGHEST = lax.Precision.HIGHEST
NT = (((1,), (1,)), ((), ()))
NN = (((1,), (0,)), ((), ()))


def each(count, body):
    if count <= 8:
        for index in range(count):
            body(index)
    else:
        lax.fori_loop(0, count, lambda index, carry: (body(index), carry)[1], 0)


def flipped(cell, bits, count):
    bit = 1
    while bit < count:
        own = lax.rem(cell // bit, 2)
        cell = cell + (bits // bit % 2) * (bit - 2 * bit * own)
        bit *= 2
    return cell


def halves(value):
    high = value.astype(BF16)
    low = (value - high.astype(F32)).astype(BF16)
    return high, low


def stacked(value):
    return jnp.concatenate(halves(value), axis=0)


def dot3(small, high, low, dims):
    rows = small.shape[0] // 2
    both = lax.dot_general(small, high, dims, preferred_element_type=F32)
    rest = lax.dot_general(small[:rows], low, dims, preferred_element_type=F32)
    return both[:rows] + (both[rows:] + rest)


def inverse_factor(gram):
    k = gram.shape[0]
    row_ids = lax.broadcasted_iota(jnp.int32, gram.shape, 0)
    lanes = lax.broadcasted_iota(jnp.int32, gram.shape, 1)
    start = jnp.where(lanes < k, (lanes == row_ids).astype(F32), gram)
    step = 8
    blocks = [start[i : i + step] for i in range(0, k, step)]
    ids = lax.broadcasted_iota(jnp.int32, (step, gram.shape[1]), 0)

    def spread(block, lane):
        return jnp.broadcast_to(block[:, lane : lane + 1], block.shape)

    for b in range(k // step):
        first = k + step * b
        block = blocks[b]
        pivot_columns = [spread(block, first + r) for r in range(step)]
        reciprocals = []
        for r in range(step):
            reciprocals.append(1.0 / pivot_columns[r][r : r + 1])
            ratio = jnp.where(ids > r, pivot_columns[r], 0.0) * reciprocals[r]
            block = block - ratio * block[r : r + 1]
            for j in range(r + 1, step):
                pivot_columns[j] = pivot_columns[j] - ratio * pivot_columns[j][r : r + 1]
        for i in range(b + 1, k // step):
            columns = [spread(blocks[i], first + r) for r in range(step)]
            below = blocks[i]
            for r in range(step):
                ratio = columns[r] * reciprocals[r]
                below = below - ratio * block[r : r + 1]
                for j in range(r + 1, step):
                    columns[j] = columns[j] - ratio * pivot_columns[j][r : r + 1]
            blocks[i] = below
        blocks[b] = block
    full = jnp.concatenate(blocks, axis=0)
    pivots = jnp.sum(jnp.where(lanes - k == row_ids, full, 0.0), axis=1, keepdims=True)
    return full / jnp.sqrt(pivots)


def kernel(
    n, owners, chunk, splits, data, sketch, out, stage, drawn, high, low, high_t, low_t, small, parts, inbox, gathered, acc, grams, total, inverse,
    load_sem, drawn_sem, part_send, part_recv, gather_send, gather_recv, gram_send, gram_recv, inv_send, inv_recv,
):
    me, side = lax.axis_index("cells"), lax.axis_index("side")
    genes, width = data.shape[1:]
    k = sketch.shape[0]
    rows = k // splits
    is_x, is_y = side == 0, side == 1
    barrier = pltpu.get_barrier_semaphore()
    paired = owners == n == 8
    loads = first_sends = second_parts = first_gathers = second_gathers = first_collect = second_collect = None
    relayed_gathers = ((),) * splits
    if paired:
        loads = ((5, 4, 7, 6, 2, 1, 3, 0), (7, 6, 5, 1, 3, 2, 4, 0))
        first_sends = (
            (5, 4, 7, 6, 2, 1, 3, 0, 13, 12, 15, 14, 10, 9, 11, 8),
            (7, 6, 5, 1, 3, 14, 2, 4, 0, 15, 13, 9, 11, 10, 12, 8),
        )
        second_parts = ((5, 4, 7, 6, 2, 3, 1, 0), (6, 1, 5, 4, 3, 2, 7, 0))
        first_gathers = ((5, 4, 7, 6, 2, 3, 1), (7, 5, 6, 4, 3, 2, 1))
        second_gathers = ((5, 4, 7, 6, 3, 2, 1), (1, 7, 6, 5, 4, 3, 2))
        first_collect = (0, 1, 2, 3, 4, 6, 7, 5)
        second_collect = (0, 1, 2, 4, 6, 3, 7, 5)
        relayed_gathers = ((5, 7), ())

    def device(cell, which):
        return {"cells": cell, "side": which}

    def cell_at(s):
        return flipped(me, s, n) if paired else lax.rem(me + s, n)

    def chunk_at(s):
        return cell_at(s) if paired else lax.rem(me + 1 + s, owners)

    def slot(s):
        return s if paired else chunk_at(s)

    def through(order, count, body, start=0, group=1):
        if order is None:
            each(count - start, lambda s: body((s + start,)))
        elif isinstance(order[0], tuple):
            inner = (me >= 2) & (me < 6)
            for test, own_order in zip((inner, jnp.logical_not(inner)), order):

                @pl.when(test)
                def _():
                    through(own_order, count, body, start, group)
        else:
            for i in range(0, len(order), group):
                body(order[i : i + group])

    def start_of(c):
        return pl.multiple_of(jnp.minimum(c * chunk, genes - chunk), 8)

    def load(s):
        return pltpu.make_async_copy(
            data.at[0, pl.ds(start_of(chunk_at(s)), chunk)], stage.at[slot(s)], load_sem.at[slot(s)]
        )

    def part_copy(h, s):
        there = s if paired else me
        return pltpu.make_async_remote_copy(
            src_ref=parts.at[h, slot(s)], dst_ref=inbox.at[h, there], send_sem=part_send.at[h, slot(s)],
            recv_sem=part_recv.at[h, there], device_id=device(chunk_at(s), 1 - side), device_id_type=MESH,
        )

    def part_arrival(h, s):
        here = s if paired else cell_at(s)
        pltpu.make_async_remote_copy(
            src_ref=parts.at[h, 0], dst_ref=inbox.at[h, here], send_sem=part_send.at[h, 0],
            recv_sem=part_recv.at[h, here], device_id=device(cell_at(s), 1 - side), device_id_type=MESH,
        ).wait_recv()
        return inbox[h, here]

    own = 0 if paired else me

    def gather_copy(h, s):
        there = s if paired else me
        return pltpu.make_async_remote_copy(
            src_ref=gathered.at[h, own], dst_ref=gathered.at[h, there], send_sem=gather_send.at[h, s],
            recv_sem=gather_recv.at[h, there], device_id=device(cell_at(s), side), device_id_type=MESH,
        )

    def gather_arrival(h, here):
        pltpu.make_async_remote_copy(
            src_ref=gathered.at[h, here], dst_ref=gathered.at[h, here], send_sem=gather_send.at[h, 0],
            recv_sem=gather_recv.at[h, here], device_id=device(me, side), device_id_type=MESH,
        ).wait_recv()

    def relay_gather(h, s):
        return pltpu.make_async_remote_copy(
            src_ref=gathered.at[h, s], dst_ref=gathered.at[h, s + 1], send_sem=gather_send.at[h, s + 1],
            recv_sem=gather_recv.at[h, s + 1], device_id=device(cell_at(1), side), device_id_type=MESH,
        )

    def gram_copy(cell, where, which):
        return pltpu.make_async_remote_copy(
            src_ref=grams.at[where], dst_ref=grams.at[where], send_sem=gram_send.at[which],
            recv_sem=gram_recv.at[where], device_id=device(cell, side), device_id_type=MESH,
        )

    inverse_copy = pltpu.make_async_remote_copy(
        src_ref=inverse, dst_ref=inverse, send_sem=inv_send, recv_sem=inv_recv,
        device_id=device(me, 1 - side), device_id_type=MESH,
    )

    draw = pltpu.make_async_copy(sketch, drawn, drawn_sem)
    draw.start()
    through(loads, owners, lambda group: [load(s).start() for s in group])

    @pl.when(is_x)
    def _():
        each(n, lambda s: pl.semaphore_signal(
            barrier, inc=1, device_id=device(lax.rem(me + s, n), 1 - side), device_id_type=MESH
        ))

    def prepare(s):
        value = stage[slot(s)]
        twice = owners * chunk - genes
        if twice:
            c = chunk_at(s)
            ids = lax.broadcasted_iota(jnp.int32, (twice, width), 0)
            first = jnp.where(ids >= c * chunk - start_of(c), value[:twice], 0.0)
            value = jnp.concatenate([first, value[twice:]], axis=0)
        high[slot(s)], low[slot(s)] = halves(value)

    def prepare_all(group):
        for s in group:
            load(s).wait()
        for s in group:
            prepare(s)

    def prepare_and_work_out(group):
        prepare_all(group)
        values = [dot3(small[...], high[slot(s)], low[slot(s)], NT) for s in group]
        for s, value in zip(group, values):
            for h in range(splits):
                parts[h, slot(s)] = value[h * rows : (h + 1) * rows]

    def turn(c):
        high_t[c], low_t[c] = high[c].T, low[c].T

    draw.wait()

    @pl.when(is_x)
    def _():
        through(loads, owners, prepare_all)
        each(owners, turn)

    @pl.when(is_y)
    def _():
        small[...] = stacked(drawn[...])
        through(loads, owners, prepare_and_work_out, group=4)
        pl.semaphore_wait(barrier, n)
        if paired:
            through(first_sends, splits * owners, lambda group: [part_copy(*divmod(t, owners)).start() for t in group])
        else:
            each(owners, lambda s: part_copy(0, s).start())

    def total_up(order, relayed):
        for h in range(splits):

            def add(s):
                gathered[h, own] += part_arrival(h, s)

            gathered[h, own] = part_arrival(h, 0)
            if paired:
                for s in (1, 2, 3, 6, 7, 4, 5):
                    add(s)
            else:
                each(n - 1, lambda s: add(s + 1))
            through(order, n, lambda group: [gather_copy(h, s).start() for s in group if not paired or s not in relayed[h]], 1)

    @pl.when(is_x & (me < owners))
    def _():
        total_up(first_gathers, ((),) * splits)

    @pl.when(is_y & (me < owners))
    def _():
        total_up(second_gathers, relayed_gathers)

    acc[...] = jnp.zeros_like(acc)

    def collect(h, s, relayed):
        if paired:
            c = s
            if s:
                gather_arrival(h, s)
            if s + 1 in relayed:
                relay_gather(h, s).start()
        else:
            c = lax.rem(lax.rem(me, owners) - s + owners, owners)

            @pl.when(c != me)
            def _():
                gather_arrival(h, c)

        acc[h] += dot3(stacked(gathered[h, c]), high[c], low[c], NN)

    lanes = lax.broadcasted_iota(jnp.int32, grams.shape[1:], 1)

    def work_out_gram():
        if splits == 2:
            products = lax.dot_general(small[...], small[...], NT, preferred_element_type=F32)
            pair = [products[2 * rows * h : 2 * rows * h + rows] + products[2 * rows * h + rows : 2 * rows * (h + 1)] for h in range(2)]
            top, bottom = [value + pltpu.roll(value, 2 * k - rows, axis=1) for value in pair]
            grams[me] = jnp.where(lax.rem(lanes, k) < rows, top, pltpu.roll(bottom, rows, axis=1))
            return
        range_rows = jnp.concatenate([acc[i] for i in range(splits)], axis=0)
        twice = lax.dot_general(
            range_rows, jnp.concatenate([range_rows, range_rows], axis=0), NT,
            precision=HIGHEST, preferred_element_type=F32,
        )
        grams[me] = jnp.where(lanes < k, twice[: k // 2], twice[k // 2 :])

    def send_gram():
        each(n - 1, lambda s: gram_copy(lax.rem(me + 1 + s, n), me, s).start())

    def scatter(h, group, with_gram):
        mine = small[2 * rows * h : 2 * rows * (h + 1)]
        values = [dot3(mine, high_t[slot(s)], low_t[slot(s)], NN) for s in group]
        if with_gram:
            work_out_gram()
        for s, value in zip(group, values):
            parts[h, slot(s)] = value
        if with_gram:
            send_gram()
        for s in group:
            part_copy(h, s).start()

    def scatter_all(h, order):
        for i in range(0, owners, 4):
            scatter(h, order[i : i + 4], h == splits - 1 and i == 4)

    @pl.when(is_x)
    def _():
        for h in range(splits):
            if paired:
                for s in first_collect:
                    collect(h, s, ())
            else:
                each(owners, lambda s: collect(h, s, ()))
            small[2 * rows * h : 2 * rows * (h + 1)] = stacked(acc[h])
            if paired:
                through(second_parts, owners, lambda order: scatter_all(h, order), group=owners)
            else:
                each(owners, lambda s: scatter(h, (s,), False))
        if not paired:
            work_out_gram()
            send_gram()

        def arrive(s):
            gram_copy(me, lax.rem(me - 1 - s + n, n), 0).wait_recv()

        each(n - 1, arrive)
        total[...] = grams[0]

        def add(i):
            total[...] += grams[i + 1]

        each(n - 1, add)
        top = bottom = total[...]
        if splits == 2:
            top = jnp.where(lanes < rows, top, pltpu.roll(top, k + rows, axis=1))
            bottom = jnp.where(lanes < k + rows, pltpu.roll(bottom, rows, axis=1), bottom)
        gram = jnp.concatenate([pltpu.roll(top, k, axis=1), bottom], axis=0)
        inverse[...] = inverse_factor(gram)
        inverse_copy.start()

    @pl.when(is_y)
    def _():
        for h in range(splits):
            if paired:
                for s in second_collect:
                    collect(h, s, relayed_gathers[h])
            else:
                each(owners, lambda s: collect(h, s, ()))
        inverse_copy.wait_recv()

    scale = math.sqrt(width * n)
    factor = jnp.where(is_x, scale, 1.0 / scale).astype(F32)
    full = jnp.concatenate([acc[h] for h in range(splits)], axis=0)
    out[0] = factor * dot3(stacked(inverse[:, :k]), *halves(full), NN)

    for h in range(splits):
        each(owners, lambda s: part_copy(h, s).wait_send())

        @pl.when(me < owners)
        def _():
            each(n - 1, lambda s: gather_copy(h, s + 1).wait_send())

    @pl.when(is_x)
    def _():
        each(n - 1, lambda s: gram_copy(lax.rem(me + 1 + s, n), me, s).wait_send())
        inverse_copy.wait_send()


def solution(mesh):
    n = mesh.shape["cells"]

    def per_device(datasets, sketch):
        genes, width = datasets.shape[1:]
        k = sketch.shape[0]
        chunk = 128 * -(-genes // (128 * n))
        owners = -(-genes // chunk)
        splits = 2 if owners == n == 8 and k % 16 == 0 else 1
        rows = k // splits
        dma = pltpu.SemaphoreType.DMA
        return pl.pallas_call(
            functools.partial(kernel, n, owners, chunk, splits),
            out_shape=pltpu.VMEM((1, k, width), F32),
            in_specs=[pl.BlockSpec(memory_space=pl.ANY)] * 2,
            out_specs=pl.BlockSpec(memory_space=pltpu.VMEM),
            scratch_shapes=[
                pltpu.VMEM((owners, chunk, width), F32),
                pltpu.VMEM((k, width), F32),
                pltpu.VMEM((owners, chunk, width), BF16),
                pltpu.VMEM((owners, chunk, width), BF16),
                pltpu.VMEM((owners, width, chunk), BF16),
                pltpu.VMEM((owners, width, chunk), BF16),
                pltpu.VMEM((2 * k, width), BF16),
                pltpu.VMEM((splits, owners, rows, chunk), F32),
                pltpu.VMEM((splits, n, rows, chunk), F32),
                pltpu.VMEM((splits, owners, rows, chunk), F32),
                pltpu.VMEM((splits, rows, width), F32),
                pltpu.VMEM((n, k // 2, 2 * k), F32),
                pltpu.VMEM((k // 2, 2 * k), F32),
                pltpu.VMEM((k, 2 * k), F32),
                dma((owners,)), dma,
                dma((splits, owners)), dma((splits, n)),
                dma((splits, n)), dma((splits, owners)),
                dma((n,)), dma((n,)),
                dma, dma,
            ],
            compiler_params=pltpu.CompilerParams(collective_id=0, has_side_effects=True),
            name="power_pass",
        )(datasets, sketch)

    spec = P("side", None, ("groups", "cells"))
    return jax.shard_map(
        per_device, mesh=mesh, in_specs=(spec, P(None, ("groups", "cells"))), out_specs=spec, check_vma=False
    )
```

```python
import functools
import math

import jax
import jax.numpy as jnp
from jax import lax
from jax.experimental import pallas as pl
from jax.experimental.pallas import tpu as pltpu
from jax.sharding import PartitionSpec as P

MESH = pl.DeviceIdType.MESH
F32, BF16 = jnp.float32, jnp.bfloat16
HIGHEST = lax.Precision.HIGHEST
NT = (((1,), (1,)), ((), ()))
NN = (((1,), (0,)), ((), ()))


def each(count, body):
    if count <= 8:
        for index in range(count):
            body(index)
    else:
        lax.fori_loop(0, count, lambda index, carry: (body(index), carry)[1], 0)


def flipped(cell, bits, count):
    bit = 1
    while bit < count:
        own = lax.rem(cell // bit, 2)
        cell = cell + (bits // bit % 2) * (bit - 2 * bit * own)
        bit *= 2
    return cell


def halves(value):
    high = value.astype(BF16)
    low = (value - high.astype(F32)).astype(BF16)
    return high, low


def stacked(value):
    return jnp.concatenate(halves(value), axis=0)


def dot3(small, high, low, dims):
    rows = small.shape[0] // 2
    both = lax.dot_general(small, high, dims, preferred_element_type=F32)
    rest = lax.dot_general(small[:rows], low, dims, preferred_element_type=F32)
    return both[:rows] + (both[rows:] + rest)


def inverse_factor(gram):
    k = gram.shape[0]
    row_ids = lax.broadcasted_iota(jnp.int32, gram.shape, 0)
    lanes = lax.broadcasted_iota(jnp.int32, gram.shape, 1)
    start = jnp.where(lanes < k, (lanes == row_ids).astype(F32), gram)
    step = 8
    blocks = [start[i : i + step] for i in range(0, k, step)]
    ids = lax.broadcasted_iota(jnp.int32, (step, gram.shape[1]), 0)

    def spread(block, lane):
        return jnp.broadcast_to(block[:, lane : lane + 1], block.shape)

    for b in range(k // step):
        first = k + step * b
        block = blocks[b]
        pivot_columns = [spread(block, first + r) for r in range(step)]
        reciprocals = []
        for r in range(step):
            reciprocals.append(1.0 / pivot_columns[r][r : r + 1])
            ratio = jnp.where(ids > r, pivot_columns[r], 0.0) * reciprocals[r]
            block = block - ratio * block[r : r + 1]
            for j in range(r + 1, step):
                pivot_columns[j] = pivot_columns[j] - ratio * pivot_columns[j][r : r + 1]
        for i in range(b + 1, k // step):
            columns = [spread(blocks[i], first + r) for r in range(step)]
            below = blocks[i]
            for r in range(step):
                ratio = columns[r] * reciprocals[r]
                below = below - ratio * block[r : r + 1]
                for j in range(r + 1, step):
                    columns[j] = columns[j] - ratio * pivot_columns[j][r : r + 1]
            blocks[i] = below
        blocks[b] = block
    full = jnp.concatenate(blocks, axis=0)
    pivots = jnp.sum(jnp.where(lanes - k == row_ids, full, 0.0), axis=1, keepdims=True)
    return full / jnp.sqrt(pivots)


def kernel(
    n, owners, chunk, splits, data, sketch, out, stage, drawn, high, low, high_t, low_t, small, parts, inbox, gathered, acc, grams, total, inverse,
    load_sem, drawn_sem, part_send, part_recv, gather_send, gather_recv, gram_send, gram_recv, inv_send, inv_recv,
):
    me, side = lax.axis_index("cells"), lax.axis_index("side")
    genes, width = data.shape[1:]
    k = sketch.shape[0]
    rows = k // splits
    is_x, is_y = side == 0, side == 1
    barrier = pltpu.get_barrier_semaphore()
    paired = owners == n == 8
    loads = first_sends = second_parts = first_gathers = second_gathers = first_collect = second_collect = None
    relayed_gathers = ((),) * splits
    if paired:
        loads = ((5, 4, 7, 6, 2, 1, 3, 0), (7, 6, 5, 1, 3, 2, 4, 0))
        first_sends = (
            (5, 4, 7, 6, 2, 1, 3, 0, 13, 12, 15, 14, 10, 9, 11, 8),
            (7, 6, 5, 1, 3, 14, 2, 4, 0, 15, 13, 9, 11, 10, 12, 8),
        )
        second_parts = ((5, 4, 7, 6, 2, 3, 1, 0), (6, 1, 5, 4, 3, 2, 7, 0))
        first_gathers = ((5, 4, 7, 6, 2, 3, 1), (7, 5, 6, 4, 3, 2, 1))
        second_gathers = ((5, 4, 7, 6, 3, 2, 1), (1, 7, 6, 5, 4, 3, 2))
        first_collect = (0, 1, 2, 3, 4, 6, 7, 5)
        second_collect = (0, 1, 2, 4, 6, 3, 7, 5)
        relayed_gathers = ((5, 7), ())

    def device(cell, which):
        return {"cells": cell, "side": which}

    def cell_at(s):
        return flipped(me, s, n) if paired else lax.rem(me + s, n)

    def chunk_at(s):
        return cell_at(s) if paired else lax.rem(me + 1 + s, owners)

    def slot(s):
        return s if paired else chunk_at(s)

    def through(order, count, body, start=0, group=1):
        if order is None:
            each(count - start, lambda s: body((s + start,)))
        elif isinstance(order[0], tuple):
            inner = (me >= 2) & (me < 6)
            for test, own_order in zip((inner, jnp.logical_not(inner)), order):

                @pl.when(test)
                def _():
                    through(own_order, count, body, start, group)
        else:
            for i in range(0, len(order), group):
                body(order[i : i + group])

    def start_of(c):
        return pl.multiple_of(jnp.minimum(c * chunk, genes - chunk), 8)

    def load(s):
        return pltpu.make_async_copy(
            data.at[0, pl.ds(start_of(chunk_at(s)), chunk)], stage.at[slot(s)], load_sem.at[slot(s)]
        )

    def part_copy(h, s):
        there = s if paired else me
        return pltpu.make_async_remote_copy(
            src_ref=parts.at[h, slot(s)], dst_ref=inbox.at[h, there], send_sem=part_send.at[h, slot(s)],
            recv_sem=part_recv.at[h, there], device_id=device(chunk_at(s), 1 - side), device_id_type=MESH,
        )

    def part_arrival(h, s):
        here = s if paired else cell_at(s)
        pltpu.make_async_remote_copy(
            src_ref=parts.at[h, 0], dst_ref=inbox.at[h, here], send_sem=part_send.at[h, 0],
            recv_sem=part_recv.at[h, here], device_id=device(cell_at(s), 1 - side), device_id_type=MESH,
        ).wait_recv()
        return inbox[h, here]

    own = 0 if paired else me

    def gather_copy(h, s):
        there = s if paired else me
        return pltpu.make_async_remote_copy(
            src_ref=gathered.at[h, own], dst_ref=gathered.at[h, there], send_sem=gather_send.at[h, s],
            recv_sem=gather_recv.at[h, there], device_id=device(cell_at(s), side), device_id_type=MESH,
        )

    def gather_arrival(h, here):
        pltpu.make_async_remote_copy(
            src_ref=gathered.at[h, here], dst_ref=gathered.at[h, here], send_sem=gather_send.at[h, 0],
            recv_sem=gather_recv.at[h, here], device_id=device(me, side), device_id_type=MESH,
        ).wait_recv()

    def relay_gather(h, s):
        return pltpu.make_async_remote_copy(
            src_ref=gathered.at[h, s], dst_ref=gathered.at[h, s + 1], send_sem=gather_send.at[h, s + 1],
            recv_sem=gather_recv.at[h, s + 1], device_id=device(cell_at(1), side), device_id_type=MESH,
        )

    def gram_copy(cell, where, which):
        return pltpu.make_async_remote_copy(
            src_ref=grams.at[where], dst_ref=grams.at[where], send_sem=gram_send.at[which],
            recv_sem=gram_recv.at[where], device_id=device(cell, side), device_id_type=MESH,
        )

    inverse_copy = pltpu.make_async_remote_copy(
        src_ref=inverse, dst_ref=inverse, send_sem=inv_send, recv_sem=inv_recv,
        device_id=device(me, 1 - side), device_id_type=MESH,
    )

    @pl.when(is_x)
    def _():
        each(n, lambda s: pl.semaphore_signal(
            barrier, inc=1, device_id=device(lax.rem(me + s, n), 1 - side), device_id_type=MESH
        ))

    draw = pltpu.make_async_copy(sketch, drawn, drawn_sem)
    draw.start()
    through(loads, owners, lambda group: [load(s).start() for s in group])

    def prepare(s):
        value = stage[slot(s)]
        twice = owners * chunk - genes
        if twice:
            c = chunk_at(s)
            ids = lax.broadcasted_iota(jnp.int32, (twice, width), 0)
            first = jnp.where(ids >= c * chunk - start_of(c), value[:twice], 0.0)
            value = jnp.concatenate([first, value[twice:]], axis=0)
        high[slot(s)], low[slot(s)] = halves(value)

    def prepare_all(group):
        for s in group:
            load(s).wait()
        for s in group:
            prepare(s)

    def prepare_and_work_out(group):
        prepare_all(group)
        values = [dot3(small[...], high[slot(s)], low[slot(s)], NT) for s in group]
        for s, value in zip(group, values):
            for h in range(splits):
                parts[h, slot(s)] = value[h * rows : (h + 1) * rows]

    def turn(c):
        high_t[c], low_t[c] = high[c].T, low[c].T

    draw.wait()

    @pl.when(is_x)
    def _():
        through(loads, owners, prepare_all)
        each(owners, turn)

    @pl.when(is_y)
    def _():
        small[...] = stacked(drawn[...])
        through(loads, owners, prepare_and_work_out, group=4)
        pl.semaphore_wait(barrier, n)
        if paired:
            through(first_sends, splits * owners, lambda group: [part_copy(*divmod(t, owners)).start() for t in group])
        else:
            each(owners, lambda s: part_copy(0, s).start())

    def total_up(order, relayed):
        for h in range(splits):

            def add(s):
                gathered[h, own] += part_arrival(h, s)

            gathered[h, own] = part_arrival(h, 0)
            if paired:
                for s in (1, 2, 3, 6, 7, 4, 5):
                    add(s)
            else:
                each(n - 1, lambda s: add(s + 1))
            through(order, n, lambda group: [gather_copy(h, s).start() for s in group if not paired or s not in relayed[h]], 1)

    @pl.when(is_x & (me < owners))
    def _():
        total_up(first_gathers, ((),) * splits)

    @pl.when(is_y & (me < owners))
    def _():
        total_up(second_gathers, relayed_gathers)

    acc[...] = jnp.zeros_like(acc)

    def collect(h, s, relayed):
        if paired:
            c = s
            if s:
                gather_arrival(h, s)
            if s + 1 in relayed:
                relay_gather(h, s).start()
        else:
            c = lax.rem(lax.rem(me, owners) - s + owners, owners)

            @pl.when(c != me)
            def _():
                gather_arrival(h, c)

        acc[h] += dot3(stacked(gathered[h, c]), high[c], low[c], NN)

    lanes = lax.broadcasted_iota(jnp.int32, grams.shape[1:], 1)

    def work_out_gram():
        if splits == 2:
            products = lax.dot_general(small[...], small[...], NT, preferred_element_type=F32)
            pair = [products[2 * rows * h : 2 * rows * h + rows] + products[2 * rows * h + rows : 2 * rows * (h + 1)] for h in range(2)]
            top, bottom = [value + pltpu.roll(value, 2 * k - rows, axis=1) for value in pair]
            grams[me] = jnp.where(lax.rem(lanes, k) < rows, top, pltpu.roll(bottom, rows, axis=1))
            return
        range_rows = jnp.concatenate([acc[i] for i in range(splits)], axis=0)
        twice = lax.dot_general(
            range_rows, jnp.concatenate([range_rows, range_rows], axis=0), NT,
            precision=HIGHEST, preferred_element_type=F32,
        )
        grams[me] = jnp.where(lanes < k, twice[: k // 2], twice[k // 2 :])

    def send_gram():
        each(n - 1, lambda s: gram_copy(lax.rem(me + 1 + s, n), me, s).start())

    def scatter(h, group, with_gram):
        mine = small[2 * rows * h : 2 * rows * (h + 1)]
        values = [dot3(mine, high_t[slot(s)], low_t[slot(s)], NN) for s in group]
        if with_gram:
            work_out_gram()
        for s, value in zip(group, values):
            parts[h, slot(s)] = value
        if with_gram:
            send_gram()
        for s in group:
            part_copy(h, s).start()

    def scatter_all(h, order):
        for i in range(0, owners, 4):
            scatter(h, order[i : i + 4], h == splits - 1 and i == 4)

    @pl.when(is_x)
    def _():
        for h in range(splits):
            if paired:
                for s in first_collect:
                    collect(h, s, ())
            else:
                each(owners, lambda s: collect(h, s, ()))
            small[2 * rows * h : 2 * rows * (h + 1)] = stacked(acc[h])
            if paired:
                through(second_parts, owners, lambda order: scatter_all(h, order), group=owners)
            else:
                each(owners, lambda s: scatter(h, (s,), False))
        if not paired:
            work_out_gram()
            send_gram()

        def arrive(s):
            gram_copy(me, lax.rem(me - 1 - s + n, n), 0).wait_recv()

        each(n - 1, arrive)
        total[...] = grams[0]

        def add(i):
            total[...] += grams[i + 1]

        each(n - 1, add)
        top = bottom = total[...]
        if splits == 2:
            top = jnp.where(lanes < rows, top, pltpu.roll(top, k + rows, axis=1))
            bottom = jnp.where(lanes < k + rows, pltpu.roll(bottom, rows, axis=1), bottom)
        gram = jnp.concatenate([pltpu.roll(top, k, axis=1), bottom], axis=0)
        inverse[...] = inverse_factor(gram)
        inverse_copy.start()

    @pl.when(is_y)
    def _():
        for h in range(splits):
            if paired:
                for s in second_collect:
                    collect(h, s, relayed_gathers[h])
            else:
                each(owners, lambda s: collect(h, s, ()))
        inverse_copy.wait_recv()

    scale = math.sqrt(width * n)
    factor = jnp.where(is_x, scale, 1.0 / scale).astype(F32)
    full = jnp.concatenate([acc[h] for h in range(splits)], axis=0)
    out[0] = factor * dot3(stacked(inverse[:, :k]), *halves(full), NN)

    for h in range(splits):
        each(owners, lambda s: part_copy(h, s).wait_send())

        @pl.when(me < owners)
        def _():
            each(n - 1, lambda s: gather_copy(h, s + 1).wait_send())

    @pl.when(is_x)
    def _():
        each(n - 1, lambda s: gram_copy(lax.rem(me + 1 + s, n), me, s).wait_send())
        inverse_copy.wait_send()


def solution(mesh):
    n = mesh.shape["cells"]

    def per_device(datasets, sketch):
        genes, width = datasets.shape[1:]
        k = sketch.shape[0]
        chunk = 128 * -(-genes // (128 * n))
        owners = -(-genes // chunk)
        splits = 2 if owners == n == 8 and k % 16 == 0 else 1
        rows = k // splits
        dma = pltpu.SemaphoreType.DMA
        return pl.pallas_call(
            functools.partial(kernel, n, owners, chunk, splits),
            out_shape=pltpu.VMEM((1, k, width), F32),
            in_specs=[pl.BlockSpec(memory_space=pl.ANY)] * 2,
            out_specs=pl.BlockSpec(memory_space=pltpu.VMEM),
            scratch_shapes=[
                pltpu.VMEM((owners, chunk, width), F32),
                pltpu.VMEM((k, width), F32),
                pltpu.VMEM((owners, chunk, width), BF16),
                pltpu.VMEM((owners, chunk, width), BF16),
                pltpu.VMEM((owners, width, chunk), BF16),
                pltpu.VMEM((owners, width, chunk), BF16),
                pltpu.VMEM((2 * k, width), BF16),
                pltpu.VMEM((splits, owners, rows, chunk), F32),
                pltpu.VMEM((splits, n, rows, chunk), F32),
                pltpu.VMEM((splits, owners, rows, chunk), F32),
                pltpu.VMEM((splits, rows, width), F32),
                pltpu.VMEM((n, k // 2, 2 * k), F32),
                pltpu.VMEM((k // 2, 2 * k), F32),
                pltpu.VMEM((k, 2 * k), F32),
                dma((owners,)), dma,
                dma((splits, owners)), dma((splits, n)),
                dma((splits, n)), dma((splits, owners)),
                dma((n,)), dma((n,)),
                dma, dma,
            ],
            compiler_params=pltpu.CompilerParams(collective_id=0, has_side_effects=True),
            name="power_pass",
        )(datasets, sketch)

    spec = P("side", None, ("groups", "cells"))
    return jax.shard_map(
        per_device, mesh=mesh, in_specs=(spec, P(None, ("groups", "cells"))), out_specs=spec, check_vma=False
    )
```
